32 devices in a mesh: tensor: 4 (over y, x), seq: 8 (over z, core).
Axes of the slice: x: 2, y: 2, z: 4, core: 2. Of those that a mesh axis runs over, the one named last changes fastest.
Arguments:
- key_states: bfloat16 [8, 2, 4096, 1024], P(None, None, 'seq', 'tensor'), may hold values from -6 to 6
- value_states: bfloat16 [8, 2, 4096, 1024], P(None, None, 'seq', 'tensor'), may hold values from -6 to 6
- bin_index: int32 [8, 8, 4096], P(None, 'tensor', 'seq'), may hold values from 0 to 4095
- retain_count: int32 [8], replicated, may hold values from 1 to 4096
Outputs:
- histogram: float32 [8, 8, 2, 4096], P(None, 'tensor', None, 'seq')
- threshold: int32 [8], replicated
The draws below stay inside these ranges and needn't reach their ends.
All inputs are finite; a program needn't handle non-finite values.
Results may differ from the reference program's by a relative error of at most 0.0029.
Values sent between devices are 32-bit elements; how exact they have to be, the bound alone decides.
A program may use at most 64 MiB of HBM per device.

```python
import jax
import jax.numpy as jnp
from jax import lax

KVH = 8
HD = 128
BINS = 4096
PAIRS = 8
TOK_DEV = 512
TOKENS = 4096


def draw_bin_index(key, part):
    blocks = TOKENS // TOK_DEV
    key_centre = jax.random.fold_in(key, 11)
    key_expo = jax.random.fold_in(key, 12)
    key_first = jax.random.fold_in(key, 13)
    key_second = jax.random.fold_in(key, 14)
    centre = jax.random.randint(key_centre, (PAIRS, KVH, blocks, 1), 0, BINS).astype(jnp.int32)
    expo = jax.random.randint(key_expo, (PAIRS, KVH, blocks, 1), 0, 8).astype(jnp.int32)
    spread = jnp.maximum(BINS // jnp.left_shift(jnp.ones_like(expo), expo), 1)
    first = jax.random.randint(key_first, (PAIRS, KVH, blocks, TOK_DEV), 0, BINS).astype(jnp.int32) % spread
    second = jax.random.randint(key_second, (PAIRS, KVH, blocks, TOK_DEV), 0, BINS).astype(jnp.int32) % spread
    placed = (centre + first + second) % BINS
    return placed.reshape(PAIRS, KVH, TOKENS).astype(jnp.int32)


def draw_retain_count(key, part):
    key_count = jax.random.fold_in(key, 21)
    highest = min(4096, TOKENS * KVH)
    return jax.random.randint(key_count, (PAIRS,), 1, highest + 1).astype(jnp.int32)


def block_scale(stream_key, shape, shards, smallest, largest):
    loudness = 1.0
    for position, blocks in shards:
        heights = jax.random.uniform(jax.random.fold_in(jax.random.fold_in(stream_key, 6), position), (blocks,), jnp.float32, smallest / len(shards), largest / len(shards))
        loudness = loudness * jnp.repeat(jnp.exp(heights), shape[position] // blocks).reshape((-1,) + (1,) * (len(shape) - 1 - position))
    return loudness


def centred(stream_key, extent, scale, bound, cuts=(), held_as=jnp.bfloat16):
    loudness = block_scale(stream_key, extent, cuts, -0.22, 0.18) if cuts else 1.0
    result = jax.random.normal(stream_key, extent, jnp.float32) * scale * loudness
    return jnp.minimum(jnp.maximum(result, -bound), bound).astype(held_as)


def setup_inputs(seed: int = 0) -> dict:
    seeds = jax.random.split(jax.random.key(seed), 5)
    return {
        "key_states": centred(seeds[0], (PAIRS, 2, TOKENS, KVH * HD), 1.0, 6.0, ((2, 8), (3, 4))),
        "value_states": centred(seeds[1], (PAIRS, 2, TOKENS, KVH * HD), 1.0, 6.0, ((2, 8), (3, 4))),
        "bin_index": draw_bin_index(jax.random.fold_in(seeds[4], 71), 0),
        "retain_count": draw_retain_count(jax.random.fold_in(seeds[4], 71), 0),
    }


def similarity(states):
    first = states[0].astype(jnp.float32).reshape(TOKENS, KVH, HD)
    second = states[1].astype(jnp.float32).reshape(TOKENS, KVH, HD)
    inner_sum = lax.optimization_barrier(jnp.sum(first * second, axis=-1))
    first_sq = lax.optimization_barrier(jnp.sum(first * first, axis=-1))
    second_sq = lax.optimization_barrier(jnp.sum(second * second, axis=-1))
    return (inner_sum / jnp.sqrt((first_sq + 1.0) * (second_sq + 1.0))).T

def one_head(weight_pair, bins_row):
    summed = jax.ops.segment_sum(weight_pair.T, bins_row, num_segments=BINS)
    counted = jax.ops.segment_sum(jnp.ones_like(weight_pair[0]), bins_row, num_segments=BINS)
    return (summed.T, counted)

def reference(key_states, value_states, bin_index, retain_count):
    key_cos = lax.map(similarity, key_states)
    value_cos = lax.map(similarity, value_states)
    rounded = jnp.stack([key_cos, value_cos], axis=2).astype(jnp.bfloat16)
    rounded = lax.optimization_barrier(rounded)
    weights = rounded.astype(jnp.float32)
    histogram, counts = jax.vmap(jax.vmap(one_head))(weights, bin_index)
    pooled = lax.optimization_barrier(jnp.sum(counts, axis=1))
    cumulative = jnp.cumsum(jnp.cumsum(pooled, axis=0), axis=1)
    target = retain_count.astype(jnp.float32)[:, None]
    threshold = lax.optimization_barrier(jnp.sum((cumulative < target).astype(jnp.int32), axis=1)).astype(jnp.int32)
    return (histogram, threshold)
```

```python
import functools

import jax
import jax.numpy as jnp
from jax import lax
from jax.experimental import pallas as pl
from jax.experimental.pallas import tpu as pltpu
from jax.sharding import PartitionSpec as P

BINS = 4096
MESH = pl.DeviceIdType.MESH
NT = (((1,), (1,)), ((), ()))
F32 = jnp.float32
BF16 = jnp.bfloat16


def iota(shape, dim):
    return lax.broadcasted_iota(jnp.int32, shape, dim)


def each(lo, hi, body):
    if hi - lo <= 8:
        for k in range(lo, hi):
            body(k)
    else:

        @pl.loop(lo, hi)
        def _(k):
            body(k)


def exact_dot(a, b):
    return jnp.dot(a, b, precision=lax.Precision.HIGHEST, preferred_element_type=F32)


def kernel(
    n, nt, key_hbm, value_hbm, bins, retain, out, threshold,
    kbuf, vbuf, lo_hot, stage_c, recv_c, mine_t, recv_t, all_x, stage_h, recv_h,
    in_sem, cs, cr, ts, tr, gs, gr, hs, hr,
):
    pairs, heads, toks = bins.shape
    width = kbuf.shape[3] // heads
    lanes = stage_c.shape[2]
    per = stage_c.shape[1] // pairs
    his = n * per
    me = lax.axis_index("seq")
    my_t = lax.axis_index("tensor")

    def loads(p):
        return (
            pltpu.make_async_copy(key_hbm.at[p], kbuf.at[p], in_sem.at[0, p]),
            pltpu.make_async_copy(value_hbm.at[p], vbuf.at[p], in_sem.at[1, p]),
        )

    for p in range(pairs):
        for c in loads(p):
            c.start()

    barrier = pltpu.get_barrier_semaphore()

    def greet(k):
        pl.semaphore_signal(barrier, inc=1, device_id={"seq": lax.rem(me + k, n)}, device_id_type=MESH)

    def greet_t(k):
        pl.semaphore_signal(barrier, inc=1, device_id={"tensor": lax.rem(my_t + k, nt)}, device_id_type=MESH)

    each(1, n, greet)
    each(1, nt, greet_t)

    shift = lanes.bit_length() - 1
    for p in range(pairs):
        count = jnp.zeros((his, lanes), F32)
        for h in range(heads):
            row = bins[p, pl.ds(h, 1), :]
            low = row & (lanes - 1)
            high = row >> shift
            lo_mat = jnp.where(iota((lanes, toks), 0) == low, 1.0, 0.0).astype(BF16)
            lo_hot[p, h] = lo_mat
            hi_mat = jnp.where(iota((his, toks), 0) == high, 1.0, 0.0).astype(BF16)
            count += lax.dot_general(hi_mat, lo_mat, NT, preferred_element_type=F32)
        for o in range(n):
            stage_c[o, pl.ds(p * per, per), :] = count[o * per:(o + 1) * per, :]

    pl.semaphore_wait(barrier, n - 1 + nt - 1)

    def copy_c(k):
        peer = lax.rem(me + k, n)
        return pltpu.make_async_remote_copy(
            src_ref=stage_c.at[peer], dst_ref=recv_c.at[k], send_sem=cs.at[k], recv_sem=cr.at[k],
            device_id={"seq": peer}, device_id_type=MESH)

    def copy_t(k):
        return pltpu.make_async_remote_copy(
            src_ref=mine_t, dst_ref=recv_t.at[k], send_sem=ts.at[k], recv_sem=tr.at[k],
            device_id={"tensor": lax.rem(my_t + k, nt)}, device_id_type=MESH)

    def copy_g(k):
        return pltpu.make_async_remote_copy(
            src_ref=all_x.at[me], dst_ref=all_x.at[me], send_sem=gs.at[k], recv_sem=gr.at[k],
            device_id={"seq": lax.rem(me + k, n)}, device_id_type=MESH)

    def copy_h(k, p):
        peer = lax.rem(me + k, n)
        return pltpu.make_async_remote_copy(
            src_ref=stage_h.at[peer, p], dst_ref=recv_h.at[k, p], send_sem=hs.at[k], recv_sem=hr.at[k],
            device_id={"seq": peer}, device_id_type=MESH)

    def copy_h_all(k):
        peer = lax.rem(me + k, n)
        return pltpu.make_async_remote_copy(
            src_ref=stage_h.at[peer], dst_ref=recv_h.at[k], send_sem=hs.at[k], recv_sem=hr.at[k],
            device_id={"seq": peer}, device_id_type=MESH)

    each(1, n, lambda k: copy_c(k).start())

    blk = 128
    eye = iota((blk, blk), 0) == iota((blk, blk), 1)

    def diag(g):
        return jnp.sum(jnp.where(eye, g, 0.0), axis=0, keepdims=True)

    def cosine(buf, p, h):
        parts = []
        for t in range(0, toks, blk):
            a = buf[p, 0, t:t + blk, h * width:(h + 1) * width]
            b = buf[p, 1, t:t + blk, h * width:(h + 1) * width]
            g = lax.dot_general(a, jnp.concatenate([a, b], axis=0), NT, preferred_element_type=F32)
            bb = diag(lax.dot_general(b, b, NT, preferred_element_type=F32))
            aa = diag(g[:, :blk])
            ab = diag(g[:, blk:])
            parts.append(ab / jnp.sqrt((aa + 1.0) * (bb + 1.0)))
        return jnp.concatenate(parts, axis=1)

    odd = (iota((2 * his, toks), 0) & 1) == 1
    hi_of = iota((2 * his, toks), 0) >> 1

    def step(p):
        for c in loads(p):
            c.wait()
        for h in range(heads):
            kc = cosine(kbuf, p, h)
            vc = cosine(vbuf, p, h)
            high = bins[p, pl.ds(h, 1), :] >> shift
            left = jnp.where(hi_of == high, jnp.where(odd, vc, kc), 0.0).astype(BF16)
            res = lax.dot_general(left, lo_hot[p, h], NT, preferred_element_type=F32)
            for o in range(n):
                stage_h[o, p, pl.ds(h * per * 2, per * 2), :] = res[o * per * 2:(o + 1) * per * 2, :]

    def send_h(p):
        each(1, n, lambda k: copy_h(k, p).start())

    third = pairs // 3

    @pl.loop(0, pairs)
    def _(p):
        step(p)
        @pl.when(p >= 1)
        def _():
            send_h(p - 1)

        @pl.when(p == third)
        def _():
            each(1, n, lambda k: copy_c(k).wait_recv())
            mine_t[...] = stage_c[me] + jnp.sum(recv_c[1:n], axis=0)
            each(1, nt, lambda k: copy_t(k).start())

        @pl.when(p == 2 * third)
        def _():
            each(1, nt, lambda k: copy_t(k).wait_recv())
            all_x[me] = mine_t[...] + jnp.sum(recv_t[1:nt], axis=0)
            each(1, n, lambda k: copy_g(k).start())

    send_h(pairs - 1)

    def wait_g(k):
        src = lax.rem(me + n - k, n)
        pltpu.make_async_remote_copy(
            src_ref=all_x.at[src], dst_ref=all_x.at[src], send_sem=gs.at[k], recv_sem=gr.at[k],
            device_id={"seq": lax.rem(me + k, n)}, device_id_type=MESH).wait_recv()

    each(1, n, wait_g)
    rows = pairs * per
    upper = jnp.where(iota((lanes, lanes), 0) <= iota((lanes, lanes), 1), 1.0, 0.0)
    r0, r1 = iota((rows, rows), 0), iota((rows, rows), 1)
    earlier = r1 // per <= r0 // per
    same = jnp.where(earlier & (r1 % per == r0 % per), 1.0, 0.0)
    before = jnp.where(earlier & (r1 % per < r0 % per), 1.0, 0.0)
    whole = jnp.where(earlier, 1.0, 0.0)
    row_pair = iota((rows, lanes), 0) // per
    goal = jnp.zeros((rows, lanes), F32)
    for p in range(pairs):
        goal = jnp.where(row_pair == p, retain[p].astype(F32), goal)

    def scan(r, carry):
        off, cnt = carry
        x = all_x[r]
        xu = exact_dot(x, upper)
        tot = jnp.broadcast_to(jnp.sum(x, axis=1, keepdims=True), (rows, lanes))
        cum = exact_dot(same, xu) + exact_dot(before, tot) + off
        cnt = cnt + jnp.where(cum < goal, 1.0, 0.0)
        return off + exact_dot(whole, tot), cnt

    zero = jnp.zeros((rows, lanes), F32)
    _, cnt = lax.fori_loop(0, n, scan, (zero, zero), unroll=n <= 8)
    for p in range(pairs):
        threshold[p] = jnp.sum(cnt[p * per:(p + 1) * per, :]).astype(jnp.int32)

    each(1, n, lambda k: copy_h_all(k).wait_recv())
    for p in range(pairs):
        acc = stage_h[me, p]
        acc = acc + jnp.sum(recv_h[1:n, p], axis=0)
        for h in range(heads):
            for j in range(per):
                at = (h * per + j) * 2
                out[p, h, :, j * lanes:(j + 1) * lanes] = acc[at:at + 2, :]

    each(1, n, lambda k: copy_c(k).wait_send())
    each(1, nt, lambda k: copy_t(k).wait_send())
    each(1, n, lambda k: copy_g(k).wait_send())
    each(1, n, lambda k: copy_h_all(k).wait_send())


def solution(mesh):
    n, nt = mesh.shape["seq"], mesh.shape["tensor"]

    def per_device(key_states, value_states, bin_index, retain_count):
        pairs, heads, toks = bin_index.shape
        span = BINS // n
        lanes = min(128, span)
        per = span // lanes
        rows = pairs * per
        vmem = pltpu.VMEM
        dma = pltpu.SemaphoreType.DMA
        return pl.pallas_call(
            functools.partial(kernel, n, nt),
            out_shape=(
                jax.ShapeDtypeStruct((pairs, heads, 2, span), F32),
                jax.ShapeDtypeStruct((pairs,), jnp.int32),
            ),
            in_specs=[
                pl.BlockSpec(memory_space=pl.ANY),
                pl.BlockSpec(memory_space=pl.ANY),
                pl.BlockSpec(memory_space=vmem),
                pl.BlockSpec(memory_space=pltpu.SMEM),
            ],
            out_specs=(pl.BlockSpec(memory_space=vmem), pl.BlockSpec(memory_space=pltpu.SMEM)),
            scratch_shapes=[
                vmem(key_states.shape, BF16),
                vmem(value_states.shape, BF16),
                vmem((pairs, heads, lanes, toks), BF16),
                vmem((n, rows, lanes), F32),
                vmem((n, rows, lanes), F32),
                vmem((rows, lanes), F32),
                vmem((nt, rows, lanes), F32),
                vmem((n, rows, lanes), F32),
                vmem((n, pairs, heads * per * 2, lanes), F32),
                vmem((n, pairs, heads * per * 2, lanes), F32),
                dma((2, pairs)),
                dma((n,)), dma((n,)), dma((nt,)), dma((nt,)),
                dma((n,)), dma((n,)), dma((n,)), dma((n,)),
            ],
            compiler_params=pltpu.CompilerParams(collective_id=0, has_side_effects=True),
        )(key_states, value_states, bin_index, retain_count)

    in_specs = (
        P(None, None, "seq", "tensor"),
        P(None, None, "seq", "tensor"),
        P(None, "tensor", "seq"),
        P(),
    )
    out_specs = (P(None, "tensor", None, "seq"), P())
    return jax.shard_map(
        per_device, mesh=mesh, in_specs=in_specs, out_specs=out_specs, check_vma=False
    )
```

```python
import functools

import jax
import jax.numpy as jnp
from jax import lax
from jax.experimental import pallas as pl
from jax.experimental.pallas import tpu as pltpu
from jax.sharding import PartitionSpec as P

BINS = 4096
MESH = pl.DeviceIdType.MESH
NT = (((1,), (1,)), ((), ()))
F32 = jnp.float32
BF16 = jnp.bfloat16


def iota(shape, dim):
    return lax.broadcasted_iota(jnp.int32, shape, dim)


def each(lo, hi, body):
    if hi - lo <= 8:
        for k in range(lo, hi):
            body(k)
    else:

        @pl.loop(lo, hi)
        def _(k):
            body(k)


def exact_dot(a, b):
    return jnp.dot(a, b, precision=lax.Precision.HIGHEST, preferred_element_type=F32)


def kernel(
    n, nt, key_hbm, value_hbm, bins, retain, out, threshold,
    kbuf, vbuf, lo_hot, stage_c, recv_c, mine_t, recv_t, all_x, stage_h, recv_d, comb, recv_h,
    in_sem, cs, cr, ts, tr, gs, gr, ds, dr, hs, hr,
):
    pairs, heads, toks = bins.shape
    width = kbuf.shape[3] // heads
    lanes = stage_c.shape[2]
    his = BINS // lanes
    per = his // n
    group, chips = 2 * nt, n // 2
    per_c = his // group
    me = lax.axis_index("seq")
    my_t = lax.axis_index("tensor")
    chip, core = me // 2, me % 2
    spot = my_t * 2 + core

    def in_plane(k):
        g = lax.rem(spot + k, group)
        return g, {"seq": chip * 2 + g % 2, "tensor": g // 2}

    def in_line(k):
        z = lax.rem(chip + k, chips)
        return z, {"seq": z * 2 + core}

    def loads(p):
        return (
            pltpu.make_async_copy(key_hbm.at[p], kbuf.at[p], in_sem.at[0, p]),
            pltpu.make_async_copy(value_hbm.at[p], vbuf.at[p], in_sem.at[1, p]),
        )

    for p in range(pairs):
        for c in loads(p):
            c.start()

    barrier = pltpu.get_barrier_semaphore()

    def greet(k):
        pl.semaphore_signal(barrier, inc=1, device_id=in_plane(k)[1], device_id_type=MESH)

    def greet_line(k):
        pl.semaphore_signal(barrier, inc=1, device_id=in_line(k)[1], device_id_type=MESH)

    each(1, group, greet)
    each(1, chips, greet_line)

    shift = lanes.bit_length() - 1
    for p in range(pairs):
        count = jnp.zeros((his, lanes), F32)
        for h in range(heads):
            row = bins[p, pl.ds(h, 1), :]
            low = row & (lanes - 1)
            high = row >> shift
            lo_mat = jnp.where(iota((lanes, toks), 0) == low, 1.0, 0.0).astype(BF16)
            lo_hot[p, h] = lo_mat
            hi_mat = jnp.where(iota((his, toks), 0) == high, 1.0, 0.0).astype(BF16)
            count += lax.dot_general(hi_mat, lo_mat, NT, preferred_element_type=F32)
        for o in range(group):
            stage_c[o, pl.ds(p * per_c, per_c), :] = count[o * per_c:(o + 1) * per_c, :]

    pl.semaphore_wait(barrier, group - 1 + chips - 1)

    def copy_c(k):
        g, device = in_plane(k)
        return pltpu.make_async_remote_copy(
            src_ref=stage_c.at[g], dst_ref=recv_c.at[k], send_sem=cs.at[k], recv_sem=cr.at[k],
            device_id=device, device_id_type=MESH)

    def copy_t(k):
        return pltpu.make_async_remote_copy(
            src_ref=mine_t, dst_ref=recv_t.at[k], send_sem=ts.at[k], recv_sem=tr.at[k],
            device_id=in_line(k)[1], device_id_type=MESH)

    def copy_g(k, slot):
        return pltpu.make_async_remote_copy(
            src_ref=all_x.at[slot], dst_ref=all_x.at[slot], send_sem=gs.at[k], recv_sem=gr.at[k],
            device_id=in_plane(k)[1], device_id_type=MESH)

    def copy_d(p):
        return pltpu.make_async_remote_copy(
            src_ref=stage_h.at[p, 1 - core], dst_ref=recv_d.at[p], send_sem=ds.at[p], recv_sem=dr.at[p],
            device_id={"seq": chip * 2 + 1 - core}, device_id_type=MESH)

    def copy_h(k, p):
        z, device = in_line(k)
        return pltpu.make_async_remote_copy(
            src_ref=comb.at[z, p], dst_ref=recv_h.at[k, p], send_sem=hs.at[k], recv_sem=hr.at[k],
            device_id=device, device_id_type=MESH)

    def copy_h_all(k):
        z, device = in_line(k)
        return pltpu.make_async_remote_copy(
            src_ref=comb.at[z], dst_ref=recv_h.at[k], send_sem=hs.at[k], recv_sem=hr.at[k],
            device_id=device, device_id_type=MESH)

    each(1, group, lambda k: copy_c(k).start())

    blk = 128
    eye = iota((blk, blk), 0) == iota((blk, blk), 1)

    def diag(g):
        return jnp.sum(jnp.where(eye, g, 0.0), axis=0, keepdims=True)

    def cosine(buf, p, h):
        parts = []
        for t in range(0, toks, blk):
            a = buf[p, 0, t:t + blk, h * width:(h + 1) * width]
            b = buf[p, 1, t:t + blk, h * width:(h + 1) * width]
            g = lax.dot_general(a, jnp.concatenate([a, b], axis=0), NT, preferred_element_type=F32)
            bb = diag(lax.dot_general(b, b, NT, preferred_element_type=F32))
            aa = diag(g[:, :blk])
            ab = diag(g[:, blk:])
            parts.append(ab / jnp.sqrt((aa + 1.0) * (bb + 1.0)))
        return jnp.concatenate(parts, axis=1)

    odd = (iota((2 * his, toks), 0) & 1) == 1
    hi_of = iota((2 * his, toks), 0) >> 1

    def step(p):
        for c in loads(p):
            c.wait()
        for h in range(heads):
            kc = cosine(kbuf, p, h)
            vc = cosine(vbuf, p, h)
            high = bins[p, pl.ds(h, 1), :] >> shift
            left = jnp.where(hi_of == high, jnp.where(odd, vc, kc), 0.0).astype(BF16)
            res = lax.dot_general(left, lo_hot[p, h], NT, preferred_element_type=F32)
            for o in range(n):
                stage_h[p, o % 2, o // 2, pl.ds(h * per * 2, per * 2), :] = res[o * per * 2:(o + 1) * per * 2, :]

    def merge(p):
        copy_d(p).wait_recv()
        comb[:, p] = stage_h[p, core] + recv_d[p]

    def send_h(p):
        each(1, chips, lambda k: copy_h(k, p).start())

    third = pairs // 3

    @pl.loop(0, pairs)
    def _(p):
        step(p)

        @pl.when(p >= 1)
        def _():
            merge(p - 1)

        copy_d(p).start()

        @pl.when(p >= 1)
        def _():
            send_h(p - 1)

        @pl.when(p == third)
        def _():
            each(1, group, lambda k: copy_c(k).wait_recv())
            mine_t[...] = stage_c[spot] + jnp.sum(recv_c[1:group], axis=0)
            each(1, chips, lambda k: copy_t(k).start())

        @pl.when(p == 2 * third + 1)
        def _():
            each(1, chips, lambda k: copy_t(k).wait_recv())
            all_x[spot] = mine_t[...] + jnp.sum(recv_t[1:chips], axis=0)
            each(1, group, lambda k: copy_g(k, spot).start())

    merge(pairs - 1)
    send_h(pairs - 1)

    each(1, group, lambda k: copy_g(k, lax.rem(spot + group - k, group)).wait_recv())
    rows = pairs * per_c
    upper = jnp.where(iota((lanes, lanes), 0) <= iota((lanes, lanes), 1), 1.0, 0.0)
    r0, r1 = iota((rows, rows), 0), iota((rows, rows), 1)
    earlier = r1 // per_c <= r0 // per_c
    same = jnp.where(earlier & (r1 % per_c == r0 % per_c), 1.0, 0.0)
    before = jnp.where(earlier & (r1 % per_c < r0 % per_c), 1.0, 0.0)
    whole = jnp.where(earlier, 1.0, 0.0)
    row_pair = iota((rows, lanes), 0) // per_c
    goal = jnp.zeros((rows, lanes), F32)
    for p in range(pairs):
        goal = jnp.where(row_pair == p, retain[p].astype(F32), goal)

    def scan(r, carry):
        off, cnt = carry
        x = all_x[r]
        xu = exact_dot(x, upper)
        tot = jnp.broadcast_to(jnp.sum(x, axis=1, keepdims=True), (rows, lanes))
        cum = exact_dot(same, xu) + exact_dot(before, tot) + off
        cnt = cnt + jnp.where(cum < goal, 1.0, 0.0)
        return off + exact_dot(whole, tot), cnt

    zero = jnp.zeros((rows, lanes), F32)
    _, cnt = lax.fori_loop(0, group, scan, (zero, zero), unroll=group <= 8)
    for p in range(pairs):
        threshold[p] = jnp.sum(cnt[p * per_c:(p + 1) * per_c, :]).astype(jnp.int32)

    each(1, chips, lambda k: copy_h_all(k).wait_recv())
    for p in range(pairs):
        acc = comb[chip, p] + jnp.sum(recv_h[1:chips, p], axis=0)
        for h in range(heads):
            for j in range(per):
                at = (h * per + j) * 2
                out[p, h, :, j * lanes:(j + 1) * lanes] = acc[at:at + 2, :]

    each(1, group, lambda k: copy_c(k).wait_send())
    each(1, chips, lambda k: copy_t(k).wait_send())
    each(1, group, lambda k: copy_g(k, spot).wait_send())
    each(0, pairs, lambda p: copy_d(p).wait_send())
    each(1, chips, lambda k: copy_h_all(k).wait_send())


def solution(mesh):
    n, nt = mesh.shape["seq"], mesh.shape["tensor"]

    def per_device(key_states, value_states, bin_index, retain_count):
        pairs, heads, toks = bin_index.shape
        span = BINS // n
        lanes = min(128, span)
        per = span // lanes
        group, chips = 2 * nt, n // 2
        rows = pairs * BINS // lanes // group
        block = (heads * per * 2, lanes)
        vmem = pltpu.VMEM
        dma = pltpu.SemaphoreType.DMA
        return pl.pallas_call(
            functools.partial(kernel, n, nt),
            out_shape=(
                jax.ShapeDtypeStruct((pairs, heads, 2, span), F32),
                jax.ShapeDtypeStruct((pairs,), jnp.int32),
            ),
            in_specs=[
                pl.BlockSpec(memory_space=pl.ANY),
                pl.BlockSpec(memory_space=pl.ANY),
                pl.BlockSpec(memory_space=vmem),
                pl.BlockSpec(memory_space=pltpu.SMEM),
            ],
            out_specs=(pl.BlockSpec(memory_space=vmem), pl.BlockSpec(memory_space=pltpu.SMEM)),
            scratch_shapes=[
                vmem(key_states.shape, BF16),
                vmem(value_states.shape, BF16),
                vmem((pairs, heads, lanes, toks), BF16),
                vmem((group, rows, lanes), F32),
                vmem((group, rows, lanes), F32),
                vmem((rows, lanes), F32),
                vmem((chips, rows, lanes), F32),
                vmem((group, rows, lanes), F32),
                vmem((pairs, 2, chips) + block, F32),
                vmem((pairs, chips) + block, F32),
                vmem((chips, pairs) + block, F32),
                vmem((chips, pairs) + block, F32),
                dma((2, pairs)),
                dma((group,)), dma((group,)), dma((chips,)), dma((chips,)),
                dma((group,)), dma((group,)), dma((pairs,)), dma((pairs,)),
                dma((chips,)), dma((chips,)),
            ],
            compiler_params=pltpu.CompilerParams(collective_id=0, has_side_effects=True),
        )(key_states, value_states, bin_index, retain_count)

    in_specs = (
        P(None, None, "seq", "tensor"),
        P(None, None, "seq", "tensor"),
        P(None, "tensor", "seq"),
        P(),
    )
    out_specs = (P(None, "tensor", None, "seq"), P())
    return jax.shard_map(
        per_device, mesh=mesh, in_specs=in_specs, out_specs=out_specs, check_vma=False
    )
```
